32 devices in a mesh: parts: 2 (over y), space: 4 (over z), tm: 2 (over x), spin: 2 (over core).
Axes of the slice: x: 2, y: 2, z: 4, core: 2. Of those that a mesh axis runs over, the one named last changes fastest.
Arguments:
- backward: bfloat16 [4, 2, 4, 64, 3, 4, 128], P('parts', 'tm', None, 'spin', None, 'space'), parts along dimension 0, may hold values from -6 to 6
- forward: bfloat16 [4, 2, 4, 64, 3, 4, 128], P('parts', 'tm', None, 'spin', None, 'space'), parts along dimension 0, may hold values from -6 to 6
- gauge_links: bfloat16 [4, 3, 3, 3, 2, 4, 128], P('parts', None, None, None, 'tm', 'space'), parts along dimension 0, may hold values from -2.5 to 2.5
- momenta: int32 [3, 3], replicated, may hold values from -2 to 2
- gamma_list: int32 [16], replicated, may hold values from 0 to 15
Outputs:
- insertion: float32 [4, 3, 16, 2, 64, 64], P('parts', None, None, 'tm', 'space', 'spin'), parts along dimension 0
The draws below stay inside these ranges and needn't reach their ends.
There are 2 independent parts, one for each index of `parts`. The reference program is written for one: setup_inputs(seed, part) draws one part's arguments, and reference() takes and returns one part's arrays. A program takes and returns all parts, laid end to end along the dimension named above; an argument that names none is the same for every part. Nothing has to cross between parts.
All inputs are finite; a program needn't handle non-finite values.
Results may differ from the reference program's by a relative error of at most 0.0056.
Values may be sent and summed in bfloat16 or wider, within the bound.
No kernel may reach another device: no remote copies, remote signals or barrier semaphores. Data moves between devices by JAX's collectives and lax.ppermute only.
A program may use at most 64 MiB of HBM per device.

```python
import math
import jax
import jax.numpy as jnp
import numpy as np
from jax import lax

LX = 32
LY = 4
NCOL = 64
NGAM = 16
NMOM = 3
LZ = 4
SLAB = 2


def with_ends(values, rng, low, top_value):
    index_at = [jax.random.randint(jax.random.fold_in(rng, axis), (), 0, length) for axis, length in enumerate(values.shape)]
    widest = values.shape.index(max(values.shape))
    neighbour = index_at[:widest] + [(index_at[widest] + 1) % values.shape[widest]] + index_at[widest + 1:]
    return values.at[tuple(index_at)].set(low).at[tuple(neighbour)].set(top_value)


def block_scale(stream_key, extent, cuts, low, high):
    factor_of = 1.0
    for axis_at, parts in cuts:
        draws = jax.random.uniform(jax.random.fold_in(jax.random.fold_in(stream_key, 6), axis_at), (parts,), jnp.float32, low / len(cuts), high / len(cuts))
        factor_of = factor_of * jnp.repeat(jnp.exp(draws), extent[axis_at] // parts).reshape((-1,) + (1,) * (len(extent) - 1 - axis_at))
    return factor_of


def bell_draw(rng, extent, width, reach, split=(), kind=jnp.bfloat16):
    entries = width * jax.random.normal(rng, extent, jnp.float32)
    if split:
        entries = entries * block_scale(rng, extent, split, -0.22, 0.18)
    return jnp.clip(entries, -reach, reach).astype(kind)


def setup_inputs(seed: int = 0, part: int = 0) -> dict:
    splits = jax.random.split(jax.random.key(seed), 6)
    own_keys = jax.random.split(jax.random.fold_in(splits[5], part), 6)
    return {
        "backward": bell_draw(own_keys[0], (2, SLAB, 4, NCOL, 3, LZ, LX * LY), 1.0, 6.0, ((1, 2), (3, 2), (5, 4))),
        "forward": bell_draw(own_keys[1], (2, SLAB, 4, NCOL, 3, LZ, LX * LY), 1.0, 6.0, ((1, 2), (3, 2), (5, 4))),
        "gauge_links": bell_draw(own_keys[2], (2, 3, 3, 3, SLAB, LZ, LX * LY), 0.41, 2.5, ((4, 2), (5, 4))),
        "momenta": with_ends(jax.random.randint(splits[3], (NMOM, 3), -2, 3), jax.random.fold_in(splits[3], 1), -2, 2).astype(jnp.int32),
        "gamma_list": with_ends(jax.random.randint(splits[4], (NGAM,), 0, 16), jax.random.fold_in(splits[4], 1), 0, 15).astype(jnp.int32),
    }


def gamma_tables():
    zeros = np.zeros((4, 4))
    gx_imag = np.array([[0, 0, 0, 1], [0, 0, 1, 0], [0, -1, 0, 0], [-1, 0, 0, 0]]) * 1.0
    gy_real = np.array([[0, 0, 0, -1], [0, 0, 1, 0], [0, 1, 0, 0], [-1, 0, 0, 0]]) * 1.0
    gz_imag = np.array([[0, 0, 1, 0], [0, 0, 0, -1], [-1, 0, 0, 0], [0, 1, 0, 0]]) * 1.0
    gt_real = np.array([[0, 0, 1, 0], [0, 0, 0, 1], [1, 0, 0, 0], [0, 1, 0, 0]]) * 1.0
    singles = [(zeros, gx_imag), (gy_real, zeros), (zeros, gz_imag), (gt_real, zeros)]
    clif_real = []
    clif_imag = []
    for number in range(16):
        mat_real = np.eye(4)
        mat_imag = np.zeros((4, 4))
        for which in range(4):
            if number >> which & 1:
                other_real, other_imag = singles[which]
                new_real = mat_real @ other_real - mat_imag @ other_imag
                new_imag = mat_real @ other_imag + mat_imag @ other_real
                mat_real, mat_imag = (new_real, new_imag)
        clif_real.append(mat_real)
        clif_imag.append(mat_imag)
    return (singles, (np.stack(clif_real), np.stack(clif_imag)))

def chosen_gammas(gamma_list):
    singles, clifford = gamma_tables()
    table_real = jnp.asarray(clifford[0], dtype=jnp.float32)
    table_imag = jnp.asarray(clifford[1], dtype=jnp.float32)
    one_hot = (gamma_list[:, None] == jnp.arange(16, dtype=jnp.int32)[None, :]).astype(jnp.float32)
    gam_real = jnp.einsum('kg,gsv->ksv', one_hot, table_real, precision=lax.Precision.HIGHEST)
    gam_imag = jnp.einsum('kg,gsv->ksv', one_hot, table_imag, precision=lax.Precision.HIGHEST)
    return (gam_real, gam_imag)

def color_apply(link_real, link_imag, spin_real, spin_imag, dagger):
    outs_real = []
    outs_imag = []
    for c in range(3):
        summed_real = 0.0
        summed_imag = 0.0
        for d in range(3):
            if dagger:
                coef_real = link_real[d, c]
                coef_imag = -link_imag[d, c]
            else:
                coef_real = link_real[c, d]
                coef_imag = link_imag[c, d]
            coef_real = coef_real[..., None, None, :, :]
            coef_imag = coef_imag[..., None, None, :, :]
            part_real = spin_real[..., d, :, :]
            part_imag = spin_imag[..., d, :, :]
            summed_real = summed_real + coef_real * part_real - coef_imag * part_imag
            summed_imag = summed_imag + coef_real * part_imag + coef_imag * part_real
        outs_real.append(summed_real)
        outs_imag.append(summed_imag)
    return (jnp.stack(outs_real, axis=-3), jnp.stack(outs_imag, axis=-3))

def spin_apply(matrix, spin_real, spin_imag):
    outs_real = []
    outs_imag = []
    for t in range(4):
        summed_real = 0.0
        summed_imag = 0.0
        for s in range(4):
            coef_real = float(matrix[0][t, s])
            coef_imag = float(matrix[1][t, s])
            if coef_real == 0.0 and coef_imag == 0.0:
                continue
            part_real = spin_real[..., s, :, :, :, :]
            part_imag = spin_imag[..., s, :, :, :, :]
            summed_real = summed_real + coef_real * part_real - coef_imag * part_imag
            summed_imag = summed_imag + coef_real * part_imag + coef_imag * part_real
        outs_real.append(summed_real)
        outs_imag.append(summed_imag)
    return (jnp.stack(outs_real, axis=-5), jnp.stack(outs_imag, axis=-5))

def plane_roll(spinor, offset, along_y, width_x):
    initial = spinor.shape
    gridded = spinor.reshape(initial[:-1] + (initial[-1] // width_x, width_x))
    gridded = jnp.roll(gridded, offset, axis=-2 if along_y else -1)
    return gridded.reshape(initial)

def current(fwd_real, fwd_imag, link_real, link_imag, up_z, down_z, width_x):
    singles, clifford = gamma_tables()
    summed_real = 0.0
    summed_imag = 0.0
    for direction in range(3):
        single_real, single_imag = singles[direction]
        minus_proj = ((np.eye(4) - single_real) / 2.0, -single_imag / 2.0)
        plus_proj = ((np.eye(4) + single_real) / 2.0, single_imag / 2.0)
        if direction < 2:
            along_y = direction == 1
            up_real = plane_roll(fwd_real, -1, along_y, width_x)
            up_imag = plane_roll(fwd_imag, -1, along_y, width_x)
            back_real, back_imag = color_apply(link_real[direction], link_imag[direction], fwd_real, fwd_imag, True)
            down_real = plane_roll(back_real, 1, along_y, width_x)
            down_imag = plane_roll(back_imag, 1, along_y, width_x)
        else:
            up_real, up_imag = up_z
            down_real, down_imag = down_z
        hop_real, hop_imag = color_apply(link_real[direction], link_imag[direction], up_real, up_imag, False)
        ahead_real, ahead_imag = spin_apply(minus_proj, hop_real, hop_imag)
        behind_real, behind_imag = spin_apply(plus_proj, down_real, down_imag)
        summed_real = summed_real + ahead_real - behind_real
        summed_imag = summed_imag + ahead_imag - behind_imag
    return (summed_real, summed_imag)

def phase_list(momenta, z_start, layers, plane_size, width_x, width_y, full_z):
    sites = jnp.arange(plane_size, dtype=jnp.int32)
    coord_x = sites % width_x
    coord_y = sites // width_x
    coord_z = z_start + jnp.arange(layers, dtype=jnp.int32)
    result = []
    for number in range(momenta.shape[0]):
        frac_plane = jnp.mod(momenta[number, 0] * coord_x, width_x).astype(jnp.float32) / float(width_x)
        frac_plane = frac_plane + jnp.mod(momenta[number, 1] * coord_y, width_y).astype(jnp.float32) / float(width_y)
        frac_depth = jnp.mod(momenta[number, 2] * coord_z, full_z).astype(jnp.float32) / float(full_z)
        result.append(2.0 * math.pi * (frac_depth[:, None] + frac_plane[None, :]))
    return result

def contract(back_piece, weave_re, weave_im, thetas, gam_real, gam_imag, scaling):
    back_real = back_piece[0].astype(jnp.float32)
    back_imag = back_piece[1].astype(jnp.float32)
    slab_times, spins, columns = (back_real.shape[0], back_real.shape[1], back_real.shape[2])
    blocks = []
    for theta in thetas:
        cosine = jnp.cos(theta)
        sine_part = jnp.sin(theta)
        rot_real = lax.optimization_barrier((cosine * back_real - sine_part * back_imag).astype(jnp.bfloat16)).astype(jnp.float32)
        rot_imag = lax.optimization_barrier((sine_part * back_real + cosine * back_imag).astype(jnp.bfloat16)).astype(jnp.float32)
        stacked = jnp.concatenate([rot_real.reshape(slab_times, spins, columns, -1), rot_imag.reshape(slab_times, spins, columns, -1)], axis=-1)
        pair_real = jnp.einsum('usak,uvbk->usvab', stacked, weave_re)
        pair_imag = jnp.einsum('usak,uvbk->usvab', stacked, weave_im)
        out_real = jnp.einsum('ksv,usvab->kuab', gam_real, pair_real, precision=lax.Precision.HIGHEST) - jnp.einsum('ksv,usvab->kuab', gam_imag, pair_imag, precision=lax.Precision.HIGHEST)
        out_imag = jnp.einsum('ksv,usvab->kuab', gam_real, pair_imag, precision=lax.Precision.HIGHEST) + jnp.einsum('ksv,usvab->kuab', gam_imag, pair_real, precision=lax.Precision.HIGHEST)
        blocks.append(jnp.stack([out_real, out_imag]) * scaling)
    return jnp.stack(blocks, axis=1)

def reference(backward, forward, gauge_links, momenta, gamma_list):
    layers = forward.shape[5]
    plane_size = forward.shape[6]
    width_x = LX
    thetas = phase_list(momenta, jnp.int32(0), layers, plane_size, width_x, plane_size // width_x, layers)
    gam_real, gam_imag = chosen_gammas(gamma_list)
    scaling = 1.0 / math.sqrt(3.0 * plane_size * layers)

    def one_time(slices):
        back_slice, fwd_slice, link_slice = slices
        fwd_real = fwd_slice[0][None].astype(jnp.float32)
        fwd_imag = fwd_slice[1][None].astype(jnp.float32)
        link_real = link_slice[0][:, :, :, None].astype(jnp.float32)
        link_imag = link_slice[1][:, :, :, None].astype(jnp.float32)
        up_z = (jnp.roll(fwd_real, -1, axis=-2), jnp.roll(fwd_imag, -1, axis=-2))
        back_real, back_imag = color_apply(link_real[2], link_imag[2], fwd_real, fwd_imag, True)
        down_z = (jnp.roll(back_real, 1, axis=-2), jnp.roll(back_imag, 1, axis=-2))
        weave_real, weave_imag = current(fwd_real, fwd_imag, link_real, link_imag, up_z, down_z, width_x)
        woven_real = lax.optimization_barrier(weave_real.astype(jnp.bfloat16)).astype(jnp.float32)
        woven_imag = lax.optimization_barrier(weave_imag.astype(jnp.bfloat16)).astype(jnp.float32)
        flat_real = woven_real.reshape(woven_real.shape[0], 4, woven_real.shape[2], -1)
        flat_imag = woven_imag.reshape(woven_imag.shape[0], 4, woven_imag.shape[2], -1)
        weave_re = jnp.concatenate([flat_real, flat_imag], axis=-1)
        weave_im = jnp.concatenate([flat_imag, -flat_real], axis=-1)
        result = contract(back_slice[:, None], weave_re, weave_im, thetas, gam_real, gam_imag, scaling)
        return result[:, :, :, 0]
    stacked = lax.map(one_time, (jnp.moveaxis(backward, 1, 0), jnp.moveaxis(forward, 1, 0), jnp.moveaxis(gauge_links, 4, 0)))
    return jnp.moveaxis(stacked, 0, 3)
```

```python
import functools
import math

import jax
import jax.numpy as jnp
import numpy as np
from jax import lax
from jax.experimental import pallas as pl
from jax.experimental.pallas import tpu as pltpu
from jax.sharding import PartitionSpec as P


LX = 32
F32 = jnp.float32
BF16 = jnp.bfloat16
VMEM = pl.BlockSpec(memory_space=pltpu.VMEM)
HBM = pl.BlockSpec(memory_space=pltpu.HBM)


def gamma_tables():
    zeros = np.zeros((4, 4))
    gx_imag = np.array([[0, 0, 0, 1], [0, 0, 1, 0], [0, -1, 0, 0], [-1, 0, 0, 0]]) * 1.0
    gy_real = np.array([[0, 0, 0, -1], [0, 0, 1, 0], [0, 1, 0, 0], [-1, 0, 0, 0]]) * 1.0
    gz_imag = np.array([[0, 0, 1, 0], [0, 0, 0, -1], [-1, 0, 0, 0], [0, 1, 0, 0]]) * 1.0
    gt_real = np.array([[0, 0, 1, 0], [0, 0, 0, 1], [1, 0, 0, 0], [0, 1, 0, 0]]) * 1.0
    singles = [zeros + 1j * gx_imag, gy_real + 0j, zeros + 1j * gz_imag, gt_real + 0j]
    basis = []
    for number in range(16):
        matrix = np.eye(4) + 0j
        for which in range(4):
            if number >> which & 1:
                matrix = matrix @ singles[which]
        basis.append(matrix)
    return (singles, basis)


SINGLES, BASIS = gamma_tables()


def unit_rows(matrix):
    columns = [int(np.flatnonzero(row)[0]) for row in matrix]
    return (columns, [complex(matrix[r, c]) for r, c in enumerate(columns)])


def plus_unit(total, unit, value):
    total_real, total_imag = total
    real, imag = value
    if unit == 1:
        return (total_real + real, total_imag + imag)
    if unit == -1:
        return (total_real - real, total_imag - imag)
    if unit == 1j:
        return (total_real - imag, total_imag + real)
    return (total_real + imag, total_imag - real)


def half_spinor(spinor, direction, sign):
    columns, units = unit_rows(SINGLES[direction])
    return [
        [plus_unit(spinor(s, c), sign * units[s], spinor(columns[s], c)) for c in range(3)]
        for s in range(2)
    ]


def colour_product(link, half, dagger):
    result = []
    for colours in half:
        row = []
        for c in range(3):
            real = imag = None
            for d in range(3):
                u_real, u_imag = link(d, c) if dagger else link(c, d)
                h_real, h_imag = colours[d]
                if dagger:
                    part_real = u_real * h_real + u_imag * h_imag
                    part_imag = u_real * h_imag - u_imag * h_real
                else:
                    part_real = u_real * h_real - u_imag * h_imag
                    part_imag = u_real * h_imag + u_imag * h_real
                real = part_real if real is None else real + part_real
                imag = part_imag if imag is None else imag + part_imag
            row.append((real, imag))
        result.append(row)
    return result


def add_hop(total, half, direction, sign, weight):
    columns, units = unit_rows(SINGLES[direction])
    for c in range(3):
        for s in range(2):
            total[s][c] = plus_unit(total[s][c], weight, half[s][c])
        for s in range(2, 4):
            total[s][c] = plus_unit(total[s][c], weight * sign * units[s], half[columns[s]][c])


def shifted(value, offset, along_y, width):
    plane = value.shape[-1]
    if along_y:
        return pltpu.roll(value, -offset * width % plane, 1)
    lane = lax.broadcasted_iota(jnp.int32, value.shape, 1) % width
    edge = width - 1 if offset == 1 else 0
    near = pltpu.roll(value, -offset % plane, 1)
    far = pltpu.roll(value, offset * (width - 1) % plane, 1)
    return jnp.where(lane == edge, far, near)


def part(real_imag, s, c):
    return (real_imag * 4 + s) * 3 + c


def half_part(real_imag, s, c):
    return (real_imag * 2 + s) * 3 + c


def link_reader(links_ref, direction):
    def link(row, column):
        pair = links_ref[(direction * 3 + row) * 3 + column].astype(F32)
        return (pair[0:1], pair[1:2])

    return link


def spinor_reader(ref, rows):
    def spinor(s, c):
        return (ref[part(0, s, c), rows].astype(F32), ref[part(1, s, c), rows].astype(F32))

    return spinor


def over_rows(count, step, body):
    def stage(number, carry):
        body(pl.ds(pl.multiple_of(number * step, step), step))
        return carry

    lax.fori_loop(0, count // step, stage, 0)


def copy_all(pairs, sems):
    copies = [pltpu.make_async_copy(*pair, sems.at[i]) for i, pair in enumerate(pairs)]
    for copy in copies:
        copy.start()
    return copies


def halo_kernel(fwd_hbm, links_hbm, up_ref, down_ref, fwd_ref, links_ref, sems):
    for copy in copy_all(((fwd_hbm, fwd_ref), (links_hbm, links_ref)), sems):
        copy.wait()
    link = link_reader(links_ref, 2)

    def rows_body(rows):
        spinor = spinor_reader(fwd_ref, rows)
        ahead = half_spinor(spinor, 2, -1)
        behind = colour_product(link, half_spinor(spinor, 2, 1), True)
        for s in range(2):
            for c in range(3):
                for ri in range(2):
                    place = half_part(ri, s, c)
                    up_ref[place, rows] = ahead[s][c][ri].astype(BF16)
                    down_ref[place, rows] = behind[s][c][ri].astype(BF16)

    over_rows(fwd_ref.shape[1], 16, rows_body)


def table_place(number):
    x = (number ^ (number >> 1)) & 1
    y = ((number >> 2) ^ (number >> 3)) & 1
    q = (number & 1) | ((number >> 2) & 1) << 1
    return 4 * q + ((3 * x) ^ (2 * y))


def local_kernel(
    momenta_hbm, own_hbm, list_hbm, fwd_ref, links_ref, other_ref,
    weave_ref, left_ref, places_ref, phase_ref, momenta_ref, own_ref, list_ref, sems,
    *, width, spaces, ordered,
):
    copies = copy_all(
        ((momenta_hbm, momenta_ref), (own_hbm, own_ref), (list_hbm, list_ref)), sems
    )
    columns, plane = fwd_ref.shape[1:]
    z_place = lax.axis_index("space")
    core = lax.axis_index("spin")

    def rows_body(rows):
        spinor = spinor_reader(fwd_ref, rows)
        total = [[(0.0, 0.0) for _ in range(3)] for _ in range(4)]
        for direction in range(2):
            link = link_reader(links_ref, direction)
            along_y = direction == 1
            half = half_spinor(spinor, direction, -1)
            half = [[tuple(shifted(v, 1, along_y, width) for v in z) for z in row] for row in half]
            add_hop(total, colour_product(link, half, False), direction, -1, 1)
            half = colour_product(link, half_spinor(spinor, direction, 1), True)
            half = [[tuple(shifted(v, -1, along_y, width) for v in z) for z in row] for row in half]
            add_hop(total, half, direction, 1, -1)
        for s in range(4):
            for c in range(3):
                for ri in range(2):
                    weave_ref[part(ri, s, c), rows] = total[s][c][ri]

    over_rows(columns, 8, rows_body)

    def whole_mod(value, modulus):
        return value - modulus * jnp.floor((value + 0.5) / modulus)

    site = lax.broadcasted_iota(jnp.int32, (1, plane), 1).astype(F32)
    row_of = jnp.floor((site + 0.5) / width)
    x_of = site - width * row_of
    height = plane // width
    for copy in copies:
        copy.wait()
    for p in range(phase_ref.shape[0]):
        mom = [momenta_ref[p, axis].astype(F32) for axis in range(3)]
        frac = whole_mod(mom[0] * x_of, width) / width + whole_mod(mom[1] * row_of, height) / height
        depth = jnp.full((1, plane), mom[2] * z_place.astype(F32), F32)
        theta = 2.0 * math.pi * (whole_mod(depth, spaces) / spaces + frac)
        phase_ref[p, 0:1] = jnp.cos(theta)
        phase_ref[p, 1:2] = jnp.sin(theta)

    for k in range(list_ref.shape[0]):
        places_ref[pl.ds(k, 1)] = jnp.full((1, places_ref.shape[1]), table_place(list_ref[k]))

    moms = phase_ref.shape[0]
    block = 2 * columns // spaces if ordered else columns

    def rotate(spinor, first, mom_step, spin_step):
        for p in range(moms):
            cosine = phase_ref[p, 0:1]
            sine = phase_ref[p, 1:2]
            for s in range(4):
                at = pl.ds(pl.multiple_of(first + p * mom_step + s * spin_step, block), block)
                for c in range(3):
                    real, imag = spinor(s, c)
                    lanes = pl.ds(c * plane, plane)
                    left_ref[at, lanes] = (cosine * real - sine * imag).astype(BF16)
                    lanes = pl.ds((3 + c) * plane, plane)
                    left_ref[at, lanes] = (sine * real + cosine * imag).astype(BF16)

    for source_ref, half in ((own_ref, core), (other_ref, 1 - core)):
        for number in range(columns // block):
            spinor = spinor_reader(source_ref, pl.ds(number * block, block))
            if ordered:
                k = (half * (columns // block) + number - z_place + spaces) % spaces
                rotate(spinor, k * moms * 4 * block, 4 * block, block)
            else:
                rotate(spinor, half * columns, 8 * columns, 2 * columns)


def multiply(left_ref, right_ref, outs, first_block, moms):
    height = outs[0].shape[0]
    wide = right_ref.shape[0]
    share = moms * height
    pairs = lax.dot_general(
        left_ref[pl.ds(first_block * share, len(outs) * share)],
        right_ref[...],
        (((1,), (1,)), ((), ())),
        preferred_element_type=F32,
    )
    for number, out_ref in enumerate(outs):
        for p in range(moms):
            first = number * share + p * height
            out_ref[:, pl.ds(p * wide, wide)] = pairs[first : first + height].astype(out_ref.dtype)


def first_pairs_kernel(
    weave_ref, ahead_ref, behind_ref, links_ref, left_ref, right_ref, out_ref, *, first_block, moms
):
    columns, plane = weave_ref.shape[1:]
    wide = 4 * columns
    link = link_reader(links_ref, 2)

    def half_reader(ref, rows):
        return [
            [tuple(ref[half_part(ri, s, c), rows].astype(F32) for ri in range(2)) for c in range(3)]
            for s in range(2)
        ]

    def rows_body(rows):
        total = [
            [(weave_ref[part(0, s, c), rows], weave_ref[part(1, s, c), rows]) for c in range(3)]
            for s in range(4)
        ]
        add_hop(total, colour_product(link, half_reader(ahead_ref, rows), False), 2, -1, 1)
        add_hop(total, half_reader(behind_ref, rows), 2, 1, -1)
        for s in range(4):
            at_real = pl.ds(pl.multiple_of(s * columns + rows.start, 8), rows.size)
            at_imag = pl.ds(pl.multiple_of(wide + s * columns + rows.start, 8), rows.size)
            for c in range(3):
                real, imag = total[s][c]
                first = pl.ds(c * plane, plane)
                second = pl.ds((3 + c) * plane, plane)
                right_ref[at_real, first] = real.astype(BF16)
                right_ref[at_real, second] = imag.astype(BF16)
                right_ref[at_imag, first] = imag.astype(BF16)
                right_ref[at_imag, second] = (-real).astype(BF16)

    over_rows(columns, 8, rows_body)
    multiply(left_ref, right_ref, [out_ref], first_block, moms)


def other_pairs_kernel(left_ref, right_ref, own_ref, *out_refs, moms):
    multiply(left_ref, right_ref, [own_ref], 0, moms)
    if out_refs:
        multiply(left_ref, right_ref, out_refs, 2, moms)


def insertion_kernel(places_ref, *rest, scaling):
    *in_refs, out_hbm, table_ref, out_ref, sems = rest
    moms, _, count, block, columns = out_ref.shape
    wide = 4 * columns
    group = lax.broadcasted_iota(jnp.int32, (1, wide), 1) // columns

    def by_group(values):
        result = jnp.full((1, wide), values[0], F32)
        for j in range(1, 4):
            result = jnp.where(group == j, values[j], result)
        return result

    weights = []
    for q in range(4):
        rows = []
        for s in range(4):
            units = []
            for j in range(4):
                x, y = {0: (0, 0), 3: (1, 0), 2: (0, 1), 1: (1, 1)}[j]
                first, third = q & 1, q >> 1
                number = first | (first ^ x) << 1 | third << 2 | (third ^ y) << 3
                units.append(complex(BASIS[number][s, s ^ j]) * scaling)
            rows.append((by_group([u.real for u in units]), by_group([u.imag for u in units])))
        weights.append(rows)

    even = group % 2 == 0

    def crossed(value, s):
        if s & 1:
            value = jnp.where(
                even, pltpu.roll(value, wide - columns, 1), pltpu.roll(value, columns, 1)
            )
        if s & 2:
            value = pltpu.roll(value, 2 * columns, 1)
        return value

    places = [places_ref[pl.ds(k, 1), pl.ds(0, 1)][0, 0] for k in range(count)]

    def one_momentum(p):
        spins = []
        for s in range(4):
            both = []
            for ri in range(2):
                lanes = pl.ds((2 * p + ri) * wide, wide)
                total = None
                for ref in in_refs:
                    for lead in range(ref.shape[0]):
                        term = ref[lead, pl.ds(s * block, block), lanes].astype(F32)
                        total = term if total is None else total + term
                both.append(crossed(total, s))
            spins.append(both)
        for q in range(4):
            real = imag = None
            for s in range(4):
                w_real, w_imag = weights[q][s]
                a, b = spins[s]
                part_real = w_real * a - w_imag * b
                part_imag = w_real * b + w_imag * a
                real = part_real if real is None else real + part_real
                imag = part_imag if imag is None else imag + part_imag
            for j in range(4):
                for ri, value in enumerate((real, imag)):
                    if j:
                        value = pltpu.roll(value, wide - j * columns, 1)
                    table_ref[p, 4 * q + j, ri] = value[:, :columns]
        for k in range(count):
            for ri in range(2):
                out_ref[p, ri, k] = table_ref[p, places[k], ri]
        output_copy(p).start()

    def output_copy(p):
        return pltpu.make_async_copy(out_ref.at[p], out_hbm.at[:, p], sems.at[p])

    for p in range(moms):
        one_momentum(p)
    for p in range(moms):
        output_copy(p).wait()


def passed_along(value, axis, steps):
    count = lax.axis_size(axis)
    pairs = [(source, (source + steps) % count) for source in range(count)]
    return lax.ppermute(value, axis, pairs)


def call(kernel, out_shape, ins, cost, outs=VMEM, **kwargs):
    many = isinstance(out_shape, (list, tuple))
    return pl.pallas_call(
        kernel,
        out_shape=out_shape,
        in_specs=ins,
        out_specs=[outs] * len(out_shape) if many else outs,
        compiler_params=pltpu.CompilerParams(vmem_limit_bytes=16 * 2**20),
        cost_estimate=pl.CostEstimate(flops=cost, bytes_accessed=2**20, transcendentals=0),
        **kwargs,
    )


def in_hbm(value):
    return pltpu.with_memory_space_constraint(value, pltpu.HBM)


def shape(dims, dtype):
    return jax.ShapeDtypeStruct(dims, dtype)


def body(backward, forward, gauge_links, momenta, gamma_list):
    _, times, _, columns, _, layers, plane = forward.shape
    assert times == 1 and layers == 1
    spaces = lax.axis_size("space")
    moms = momenta.shape[0]
    count = gamma_list.shape[0]
    block = 2 * columns // spaces
    ordered = block % 16 == 0
    fwd = jnp.transpose(forward, (0, 1, 2, 4, 5, 3, 6)).reshape(24, columns, plane)
    own = jnp.transpose(backward, (0, 1, 2, 4, 5, 3, 6)).reshape(24, columns, plane)
    links = jnp.transpose(gauge_links, (1, 2, 3, 4, 5, 0, 6)).reshape(27, 2, plane)

    other = passed_along(own, "spin", 1)
    half = shape((12, columns, plane), BF16)
    to_up, to_down, fwd_here, links_here = call(
        halo_kernel,
        [half, half] + [shape(v.shape, v.dtype) for v in (fwd, links)],
        [HBM] * 2,
        10**7,
        scratch_shapes=[pltpu.SemaphoreType.DMA((2,))],
    )(*[in_hbm(v) for v in (fwd, links)])
    behind = passed_along(to_down, "space", 1)
    ahead = passed_along(to_up, "space", -1)
    rows = 8 * columns
    weave, left, places = call(
        functools.partial(local_kernel, width=LX, spaces=spaces, ordered=ordered),
        [
            shape((24, columns, plane), F32),
            shape((moms * rows, 6 * plane), BF16),
            shape((count, plane), jnp.int32),
        ],
        [HBM, HBM, HBM, VMEM, VMEM, VMEM],
        10**8,
        scratch_shapes=[
            pltpu.VMEM((moms, 2, plane), F32),
            pltpu.SMEM(momenta.shape, jnp.int32),
            pltpu.VMEM(own.shape, BF16),
            pltpu.SMEM(gamma_list.shape, jnp.int32),
            pltpu.SemaphoreType.DMA((3,)),
        ],
    )(in_hbm(momenta), in_hbm(own), in_hbm(gamma_list), fwd_here, links_here, other)
    wide = 8 * columns
    share = rows // spaces if ordered else rows
    pair_shape = shape((share, moms * wide), BF16)
    right, first = call(
        functools.partial(first_pairs_kernel, first_block=int(ordered), moms=moms),
        [shape((wide, 6 * plane), BF16), pair_shape],
        [VMEM] * 5,
        10**9,
    )(weave, ahead, behind, links_here, left)
    if ordered:
        own_pairs, *others = call(
            functools.partial(other_pairs_kernel, moms=moms),
            [shape(pair_shape.shape, F32)] + [pair_shape] * (spaces - 2),
            [VMEM] * 2,
            10**9,
        )(left, right)
        blocks = [own_pairs]
        for k, value in enumerate([first, *others], 1):
            blocks.append(passed_along(value, "space", k))
        blocks = [b[None] for b in blocks]
    else:
        split = first.reshape(4, spaces, block, moms * wide)
        split = jnp.swapaxes(split, 0, 1).reshape(spaces, 4 * block, moms * wide)
        blocks = [lax.all_to_all(split, "space", 0, 0, tiled=True)]
    scaling = 0.5 / math.sqrt(3.0 * plane * spaces)
    result = call(
        functools.partial(insertion_kernel, scaling=scaling),
        shape((2, moms, count, block, columns), F32),
        [VMEM] + [VMEM] * len(blocks),
        10**8,
        outs=HBM,
        scratch_shapes=[
            pltpu.VMEM((moms, 16, 2, block, columns), F32),
            pltpu.VMEM((moms, 2, count, block, columns), F32),
            pltpu.SemaphoreType.DMA((moms,)),
        ],
    )(places, *blocks)
    return result.reshape(2, moms, count, 1, block, columns)


def solution(mesh):
    in_specs = (
        P("parts", "tm", None, "spin", None, "space", None),
        P("parts", "tm", None, "spin", None, "space", None),
        P("parts", None, None, None, "tm", "space", None),
        P(),
        P(),
    )
    out_specs = P("parts", None, None, "tm", "space", "spin")
    return jax.shard_map(body, mesh=mesh, in_specs=in_specs, out_specs=out_specs, check_vma=False)
```

```python
import functools
import math

import jax
import jax.numpy as jnp
import numpy as np
from jax import lax
from jax.experimental import pallas as pl
from jax.experimental.pallas import tpu as pltpu
from jax.sharding import PartitionSpec as P


LX = 32
F32 = jnp.float32
BF16 = jnp.bfloat16
VMEM = pl.BlockSpec(memory_space=pltpu.VMEM)
HBM = pl.BlockSpec(memory_space=pltpu.HBM)


def gamma_tables():
    zeros = np.zeros((4, 4))
    gx_imag = np.array([[0, 0, 0, 1], [0, 0, 1, 0], [0, -1, 0, 0], [-1, 0, 0, 0]]) * 1.0
    gy_real = np.array([[0, 0, 0, -1], [0, 0, 1, 0], [0, 1, 0, 0], [-1, 0, 0, 0]]) * 1.0
    gz_imag = np.array([[0, 0, 1, 0], [0, 0, 0, -1], [-1, 0, 0, 0], [0, 1, 0, 0]]) * 1.0
    gt_real = np.array([[0, 0, 1, 0], [0, 0, 0, 1], [1, 0, 0, 0], [0, 1, 0, 0]]) * 1.0
    singles = [zeros + 1j * gx_imag, gy_real + 0j, zeros + 1j * gz_imag, gt_real + 0j]
    basis = []
    for number in range(16):
        matrix = np.eye(4) + 0j
        for which in range(4):
            if number >> which & 1:
                matrix = matrix @ singles[which]
        basis.append(matrix)
    return (singles, basis)


SINGLES, BASIS = gamma_tables()


def unit_rows(matrix):
    columns = [int(np.flatnonzero(row)[0]) for row in matrix]
    return (columns, [complex(matrix[r, c]) for r, c in enumerate(columns)])


def plus_unit(total, unit, value):
    total_real, total_imag = total
    real, imag = value
    if unit == 1:
        return (total_real + real, total_imag + imag)
    if unit == -1:
        return (total_real - real, total_imag - imag)
    if unit == 1j:
        return (total_real - imag, total_imag + real)
    return (total_real + imag, total_imag - real)


def half_spinor(spinor, direction, sign):
    columns, units = unit_rows(SINGLES[direction])
    return [
        [plus_unit(spinor(s, c), sign * units[s], spinor(columns[s], c)) for c in range(3)]
        for s in range(2)
    ]


def colour_product(link, half, dagger):
    result = []
    for colours in half:
        row = []
        for c in range(3):
            real = imag = None
            for d in range(3):
                u_real, u_imag = link(d, c) if dagger else link(c, d)
                h_real, h_imag = colours[d]
                if dagger:
                    part_real = u_real * h_real + u_imag * h_imag
                    part_imag = u_real * h_imag - u_imag * h_real
                else:
                    part_real = u_real * h_real - u_imag * h_imag
                    part_imag = u_real * h_imag + u_imag * h_real
                real = part_real if real is None else real + part_real
                imag = part_imag if imag is None else imag + part_imag
            row.append((real, imag))
        result.append(row)
    return result


def add_hop(total, half, direction, sign, weight):
    columns, units = unit_rows(SINGLES[direction])
    for c in range(3):
        for s in range(2):
            total[s][c] = plus_unit(total[s][c], weight, half[s][c])
        for s in range(2, 4):
            total[s][c] = plus_unit(total[s][c], weight * sign * units[s], half[columns[s]][c])


def shifted(value, offset, along_y, width):
    plane = value.shape[-1]
    if along_y:
        return pltpu.roll(value, -offset * width % plane, 1)
    lane = lax.broadcasted_iota(jnp.int32, value.shape, 1) % width
    edge = width - 1 if offset == 1 else 0
    near = pltpu.roll(value, -offset % plane, 1)
    far = pltpu.roll(value, offset * (width - 1) % plane, 1)
    return jnp.where(lane == edge, far, near)


def part(real_imag, s, c):
    return (real_imag * 4 + s) * 3 + c


def half_part(real_imag, s, c):
    return (real_imag * 2 + s) * 3 + c


def link_reader(links_ref, direction):
    def link(row, column):
        pair = links_ref[(direction * 3 + row) * 3 + column].astype(F32)
        return (pair[0:1], pair[1:2])

    return link


def spinor_reader(ref, rows):
    def spinor(s, c):
        return (ref[part(0, s, c), rows].astype(F32), ref[part(1, s, c), rows].astype(F32))

    return spinor


def over_rows(count, step, body):
    def stage(number, carry):
        body(pl.ds(pl.multiple_of(number * step, step), step))
        return carry

    lax.fori_loop(0, count // step, stage, 0)


def copy_all(pairs, sems):
    copies = [pltpu.make_async_copy(*pair, sems.at[i]) for i, pair in enumerate(pairs)]
    for copy in copies:
        copy.start()
    return copies


def halo_kernel(fwd_hbm, links_hbm, up_ref, down_ref, fwd_ref, links_ref, sems):
    for copy in copy_all(((fwd_hbm, fwd_ref), (links_hbm, links_ref)), sems):
        copy.wait()
    link = link_reader(links_ref, 2)

    def rows_body(rows):
        spinor = spinor_reader(fwd_ref, rows)
        ahead = half_spinor(spinor, 2, -1)
        behind = colour_product(link, half_spinor(spinor, 2, 1), True)
        for s in range(2):
            for c in range(3):
                for ri in range(2):
                    place = half_part(ri, s, c)
                    up_ref[place, rows] = ahead[s][c][ri].astype(BF16)
                    down_ref[place, rows] = behind[s][c][ri].astype(BF16)

    over_rows(fwd_ref.shape[1], 16, rows_body)


SIGNS = [[1, 1, 1, 1], [1, -1, 1, -1], [1, 1, -1, -1], [1, -1, -1, 1]]


def unit_sum(q, j):
    x, y = {0: (0, 0), 3: (1, 0), 2: (0, 1), 1: (1, 1)}[j]
    first, third = q & 1, q >> 1
    matrix = BASIS[first | (first ^ x) << 1 | third << 2 | (third ^ y) << 3]
    values = [complex(matrix[s, s ^ j]) for s in range(4)]
    return (SIGNS.index([round((v / values[0]).real) for v in values]), values[0])


def times_unit(unit, value):
    real, imag = value
    if unit == 1:
        return (real, imag)
    if unit == -1:
        return (-real, -imag)
    return (-imag, real) if unit == 1j else (imag, -real)


def ring_place(place):
    return place ^ (place >> 1)


def table_place(number):
    x = (number ^ (number >> 1)) & 1
    y = ((number >> 2) ^ (number >> 3)) & 1
    q = (number & 1) | ((number >> 2) & 1) << 1
    return 4 * q + ((3 * x) ^ (2 * y))


def local_kernel(
    momenta_hbm, own_hbm, list_hbm, fwd_ref, links_ref, other_ref,
    weave_ref, left_ref, places_ref, phase_ref, momenta_ref, own_ref, list_ref, sems,
    *, width, spaces, ordered,
):
    copies = copy_all(
        ((momenta_hbm, momenta_ref), (own_hbm, own_ref), (list_hbm, list_ref)), sems
    )
    columns, plane = fwd_ref.shape[1:]
    z_place = lax.axis_index("space")
    core = lax.axis_index("spin")

    def rows_body(rows):
        spinor = spinor_reader(fwd_ref, rows)
        total = [[(0.0, 0.0) for _ in range(3)] for _ in range(4)]
        for direction in range(2):
            link = link_reader(links_ref, direction)
            along_y = direction == 1
            half = half_spinor(spinor, direction, -1)
            half = [[tuple(shifted(v, 1, along_y, width) for v in z) for z in row] for row in half]
            add_hop(total, colour_product(link, half, False), direction, -1, 1)
            half = colour_product(link, half_spinor(spinor, direction, 1), True)
            half = [[tuple(shifted(v, -1, along_y, width) for v in z) for z in row] for row in half]
            add_hop(total, half, direction, 1, -1)
        for s in range(4):
            for c in range(3):
                for ri in range(2):
                    weave_ref[part(ri, s, c), rows] = total[s][c][ri]

    over_rows(columns, 8, rows_body)

    def whole_mod(value, modulus):
        return value - modulus * jnp.floor((value + 0.5) / modulus)

    site = lax.broadcasted_iota(jnp.int32, (1, plane), 1).astype(F32)
    row_of = jnp.floor((site + 0.5) / width)
    x_of = site - width * row_of
    height = plane // width
    for copy in copies:
        copy.wait()
    for p in range(phase_ref.shape[0]):
        mom = [momenta_ref[p, axis].astype(F32) for axis in range(3)]
        frac = whole_mod(mom[0] * x_of, width) / width + whole_mod(mom[1] * row_of, height) / height
        depth = jnp.full((1, plane), mom[2] * z_place.astype(F32), F32)
        theta = 2.0 * math.pi * (whole_mod(depth, spaces) / spaces + frac)
        phase_ref[p, 0:1] = jnp.cos(theta)
        phase_ref[p, 1:2] = jnp.sin(theta)

    for k in range(list_ref.shape[0]):
        places_ref[pl.ds(k, 1)] = jnp.full((1, places_ref.shape[1]), table_place(list_ref[k]))

    moms = phase_ref.shape[0]
    block = 2 * columns // spaces if ordered else columns

    def rotate(spinor, first, mom_step, spin_step):
        for p in range(moms):
            cosine = phase_ref[p, 0:1]
            sine = phase_ref[p, 1:2]
            for s in range(4):
                at = pl.ds(pl.multiple_of(first + p * mom_step + s * spin_step, block), block)
                for c in range(3):
                    real, imag = spinor(s, c)
                    lanes = pl.ds(c * plane, plane)
                    left_ref[at, lanes] = (cosine * real - sine * imag).astype(BF16)
                    lanes = pl.ds((3 + c) * plane, plane)
                    left_ref[at, lanes] = (sine * real + cosine * imag).astype(BF16)

    for source_ref, half in ((own_ref, core), (other_ref, 1 - core)):
        for number in range(columns // block):
            spinor = spinor_reader(source_ref, pl.ds(number * block, block))
            if ordered:
                target = half * (columns // block) + number
                k = (ring_place(target) - ring_place(z_place) + spaces) % spaces
                k = jnp.where(k > 1, spaces + 1 - k, k)
                rotate(spinor, k * moms * 4 * block, 4 * block, block)
            else:
                rotate(spinor, half * columns, 8 * columns, 2 * columns)


def multiply(left_ref, right_ref, outs, first_block, moms):
    height = outs[0].shape[0]
    wide = right_ref.shape[0]
    share = moms * height
    pairs = lax.dot_general(
        left_ref[pl.ds(first_block * share, len(outs) * share)],
        right_ref[...],
        (((1,), (1,)), ((), ())),
        preferred_element_type=F32,
    )
    for number, out_ref in enumerate(outs):
        for p in range(moms):
            first = number * share + p * height
            out_ref[:, pl.ds(p * wide, wide)] = pairs[first : first + height].astype(out_ref.dtype)


def first_pairs_kernel(
    weave_ref, ahead_ref, behind_ref, links_ref, left_ref, right_ref, out_ref, *, first_block, moms
):
    columns, plane = weave_ref.shape[1:]
    wide = 4 * columns
    gamma_columns, units = unit_rows(SINGLES[2])
    step = 16

    def one_colour(c, links, first_row):
        rows = pl.ds(first_row, step)

        def half(ref, s, d):
            return tuple(ref[half_part(ri, s, d), rows].astype(F32) for ri in range(2))

        hops = []
        for s in range(2):
            real = imag = None
            for d in range(3):
                u_real, u_imag = links[d]
                h_real, h_imag = half(ahead_ref, s, d)
                part_real = u_real * h_real - u_imag * h_imag
                part_imag = u_real * h_imag + u_imag * h_real
                real = part_real if real is None else real + part_real
                imag = part_imag if imag is None else imag + part_imag
            back = half(behind_ref, s, c)
            hops.append((plus_unit((real, imag), -1, back), plus_unit((real, imag), 1, back)))
        for s in range(4):
            total = (weave_ref[part(0, s, c), rows], weave_ref[part(1, s, c), rows])
            if s < 2:
                real, imag = plus_unit(total, 1, hops[s][0])
            else:
                real, imag = plus_unit(total, -units[s], hops[gamma_columns[s]][1])
            at_real = pl.ds(s * columns + first_row, step)
            at_imag = pl.ds(wide + s * columns + first_row, step)
            first = pl.ds(c * plane, plane)
            second = pl.ds((3 + c) * plane, plane)
            right_ref[at_real, first] = real.astype(BF16)
            right_ref[at_real, second] = imag.astype(BF16)
            right_ref[at_imag, first] = imag.astype(BF16)
            right_ref[at_imag, second] = (-real).astype(BF16)

    link = link_reader(links_ref, 2)
    for c in range(3):
        links = [link(c, d) for d in range(3)]
        for first_row in range(0, columns, step):
            one_colour(c, links, first_row)
    multiply(left_ref, right_ref, [out_ref], first_block, moms)


def other_pairs_kernel(left_ref, right_ref, own_ref, *out_refs, moms):
    multiply(left_ref, right_ref, [own_ref], 0, moms)
    if out_refs:
        multiply(left_ref, right_ref, out_refs, 2, moms)


def insertion_kernel(places_ref, *rest, scaling):
    *in_refs, out_hbm, table_ref, out_ref, sems = rest
    moms, _, count, block, columns = out_ref.shape
    wide = 4 * columns
    group = lax.broadcasted_iota(jnp.int32, (1, wide), 1) // columns

    even = group % 2 == 0

    def crossed(value, s):
        if s & 1:
            value = jnp.where(
                even, pltpu.roll(value, wide - columns, 1), pltpu.roll(value, columns, 1)
            )
        if s & 2:
            value = pltpu.roll(value, 2 * columns, 1)
        return value

    places = [places_ref[pl.ds(k, 1), pl.ds(0, 1)][0, 0] for k in range(count)]

    def one_momentum(p):
        spins = []
        for s in range(4):
            both = []
            for ri in range(2):
                lanes = pl.ds((2 * p + ri) * wide, wide)
                total = None
                for ref in in_refs:
                    for lead in range(ref.shape[0]):
                        term = ref[lead, pl.ds(s * block, block), lanes].astype(F32)
                        total = term if total is None else total + term
                both.append(crossed(total, s))
            spins.append(both)
        sums = [[], []]
        for ri in range(2):
            a, b, c, d = (spins[s][ri] * scaling for s in range(4))
            near, far = (a + b, a - b), (c + d, c - d)
            sums[ri] = [near[0] + far[0], near[1] + far[1], near[0] - far[0], near[1] - far[1]]
        for j in range(4):
            moved = [[v if j == 0 else pltpu.roll(v, wide - j * columns, 1) for v in r] for r in sums]
            for q in range(4):
                number, unit = unit_sum(q, j)
                value = times_unit(unit, (moved[0][number], moved[1][number]))
                for ri in range(2):
                    table_ref[p, 4 * q + j, ri] = value[ri][:, :columns]
        for k in range(count):
            for ri in range(2):
                out_ref[p, ri, k] = table_ref[p, places[k], ri]
        output_copy(p).start()

    def output_copy(p):
        return pltpu.make_async_copy(out_ref.at[p], out_hbm.at[:, p], sems.at[p])

    for p in range(moms):
        one_momentum(p)
    for p in range(moms):
        output_copy(p).wait()


def passed_along(value, axis, steps):
    count = lax.axis_size(axis)
    pairs = [(source, (source + steps) % count) for source in range(count)]
    return lax.ppermute(value, axis, pairs)


def passed_around(value, axis, number):
    count = lax.axis_size(axis)
    steps = 1 if number == 1 else count + 1 - number
    at = {ring_place(device): device for device in range(count)}
    pairs = [(at[place], at[(place + steps) % count]) for place in range(count)]
    return lax.ppermute(value, axis, pairs)


def call(kernel, out_shape, ins, cost, outs=VMEM, **kwargs):
    many = isinstance(out_shape, (list, tuple))
    return pl.pallas_call(
        kernel,
        out_shape=out_shape,
        in_specs=ins,
        out_specs=[outs] * len(out_shape) if many else outs,
        compiler_params=pltpu.CompilerParams(vmem_limit_bytes=16 * 2**20),
        cost_estimate=pl.CostEstimate(flops=cost, bytes_accessed=2**20, transcendentals=0),
        **kwargs,
    )


def in_hbm(value):
    return pltpu.with_memory_space_constraint(value, pltpu.HBM)


def shape(dims, dtype):
    return jax.ShapeDtypeStruct(dims, dtype)


def body(backward, forward, gauge_links, momenta, gamma_list):
    _, times, _, columns, _, layers, plane = forward.shape
    assert times == 1 and layers == 1
    spaces = lax.axis_size("space")
    moms = momenta.shape[0]
    count = gamma_list.shape[0]
    block = 2 * columns // spaces
    ordered = block % 16 == 0
    fwd = jnp.transpose(forward, (0, 1, 2, 4, 5, 3, 6)).reshape(24, columns, plane)
    own = jnp.transpose(backward, (0, 1, 2, 4, 5, 3, 6)).reshape(24, columns, plane)
    links = jnp.transpose(gauge_links, (1, 2, 3, 4, 5, 0, 6)).reshape(27, 2, plane)

    other = passed_along(own, "spin", 1)
    half = shape((12, columns, plane), BF16)
    to_up, to_down, fwd_here, links_here = call(
        halo_kernel,
        [half, half] + [shape(v.shape, v.dtype) for v in (fwd, links)],
        [HBM] * 2,
        10**7,
        scratch_shapes=[pltpu.SemaphoreType.DMA((2,))],
    )(*[in_hbm(v) for v in (fwd, links)])
    behind = passed_along(to_down, "space", 1)
    ahead = passed_along(to_up, "space", -1)
    rows = 8 * columns
    weave, left, places = call(
        functools.partial(local_kernel, width=LX, spaces=spaces, ordered=ordered),
        [
            shape((24, columns, plane), F32),
            shape((moms * rows, 6 * plane), BF16),
            shape((count, plane), jnp.int32),
        ],
        [HBM, HBM, HBM, VMEM, VMEM, VMEM],
        10**8,
        scratch_shapes=[
            pltpu.VMEM((moms, 2, plane), F32),
            pltpu.SMEM(momenta.shape, jnp.int32),
            pltpu.VMEM(own.shape, BF16),
            pltpu.SMEM(gamma_list.shape, jnp.int32),
            pltpu.SemaphoreType.DMA((3,)),
        ],
    )(in_hbm(momenta), in_hbm(own), in_hbm(gamma_list), fwd_here, links_here, other)
    wide = 8 * columns
    share = rows // spaces if ordered else rows
    pair_shape = shape((share, moms * wide), BF16)
    right, first = call(
        functools.partial(first_pairs_kernel, first_block=int(ordered), moms=moms),
        [shape((wide, 6 * plane), BF16), pair_shape],
        [VMEM] * 5,
        10**9,
    )(weave, ahead, behind, links_here, left)
    if ordered:
        own_pairs, *others = call(
            functools.partial(other_pairs_kernel, moms=moms),
            [shape(pair_shape.shape, F32)] + [pair_shape] * (spaces - 2),
            [VMEM] * 2,
            10**9,
        )(left, right)
        blocks = [own_pairs]
        for k, value in enumerate([first, *others], 1):
            blocks.append(passed_around(value, "space", k))
        blocks = [b[None] for b in blocks]
    else:
        split = first.reshape(4, spaces, block, moms * wide)
        split = jnp.swapaxes(split, 0, 1).reshape(spaces, 4 * block, moms * wide)
        blocks = [lax.all_to_all(split, "space", 0, 0, tiled=True)]
    scaling = 0.5 / math.sqrt(3.0 * plane * spaces)
    result = call(
        functools.partial(insertion_kernel, scaling=scaling),
        shape((2, moms, count, block, columns), F32),
        [VMEM] + [VMEM] * len(blocks),
        10**8,
        outs=HBM,
        scratch_shapes=[
            pltpu.VMEM((moms, 16, 2, block, columns), F32),
            pltpu.VMEM((moms, 2, count, block, columns), F32),
            pltpu.SemaphoreType.DMA((moms,)),
        ],
    )(places, *blocks)
    return result.reshape(2, moms, count, 1, block, columns)


def solution(mesh):
    in_specs = (
        P("parts", "tm", None, "spin", None, "space", None),
        P("parts", "tm", None, "spin", None, "space", None),
        P("parts", None, None, None, "tm", "space", None),
        P(),
        P(),
    )
    out_specs = P("parts", None, None, "tm", "space", "spin")
    return jax.shard_map(body, mesh=mesh, in_specs=in_specs, out_specs=out_specs, check_vma=False)
```

```python
import functools
import math

import jax
import jax.numpy as jnp
import numpy as np
from jax import lax
from jax.experimental import pallas as pl
from jax.experimental.pallas import tpu as pltpu
from jax.sharding import PartitionSpec as P


LX = 32
F32 = jnp.float32
BF16 = jnp.bfloat16
VMEM = pl.BlockSpec(memory_space=pltpu.VMEM)
HBM = pl.BlockSpec(memory_space=pltpu.HBM)


def gamma_tables():
    zeros = np.zeros((4, 4))
    gx_imag = np.array([[0, 0, 0, 1], [0, 0, 1, 0], [0, -1, 0, 0], [-1, 0, 0, 0]]) * 1.0
    gy_real = np.array([[0, 0, 0, -1], [0, 0, 1, 0], [0, 1, 0, 0], [-1, 0, 0, 0]]) * 1.0
    gz_imag = np.array([[0, 0, 1, 0], [0, 0, 0, -1], [-1, 0, 0, 0], [0, 1, 0, 0]]) * 1.0
    gt_real = np.array([[0, 0, 1, 0], [0, 0, 0, 1], [1, 0, 0, 0], [0, 1, 0, 0]]) * 1.0
    singles = [zeros + 1j * gx_imag, gy_real + 0j, zeros + 1j * gz_imag, gt_real + 0j]
    basis = []
    for number in range(16):
        matrix = np.eye(4) + 0j
        for which in range(4):
            if number >> which & 1:
                matrix = matrix @ singles[which]
        basis.append(matrix)
    return (singles, basis)


SINGLES, BASIS = gamma_tables()


def unit_rows(matrix):
    columns = [int(np.flatnonzero(row)[0]) for row in matrix]
    return (columns, [complex(matrix[r, c]) for r, c in enumerate(columns)])


def plus_unit(total, unit, value):
    total_real, total_imag = total
    real, imag = value
    if unit == 1:
        return (total_real + real, total_imag + imag)
    if unit == -1:
        return (total_real - real, total_imag - imag)
    if unit == 1j:
        return (total_real - imag, total_imag + real)
    return (total_real + imag, total_imag - real)


def half_spinor(spinor, direction, sign):
    columns, units = unit_rows(SINGLES[direction])
    return [
        [plus_unit(spinor(s, c), sign * units[s], spinor(columns[s], c)) for c in range(3)]
        for s in range(2)
    ]


def colour_product(link, half, dagger):
    result = []
    for colours in half:
        row = []
        for c in range(3):
            real = imag = None
            for d in range(3):
                u_real, u_imag = link(d, c) if dagger else link(c, d)
                h_real, h_imag = colours[d]
                if dagger:
                    part_real = u_real * h_real + u_imag * h_imag
                    part_imag = u_real * h_imag - u_imag * h_real
                else:
                    part_real = u_real * h_real - u_imag * h_imag
                    part_imag = u_real * h_imag + u_imag * h_real
                real = part_real if real is None else real + part_real
                imag = part_imag if imag is None else imag + part_imag
            row.append((real, imag))
        result.append(row)
    return result


def add_hop(total, half, direction, sign, weight):
    columns, units = unit_rows(SINGLES[direction])
    for c in range(3):
        for s in range(2):
            total[s][c] = plus_unit(total[s][c], weight, half[s][c])
        for s in range(2, 4):
            total[s][c] = plus_unit(total[s][c], weight * sign * units[s], half[columns[s]][c])


def shifted(value, offset, along_y, width):
    plane = value.shape[-1]
    if along_y:
        return pltpu.roll(value, -offset * width % plane, 1)
    lane = lax.broadcasted_iota(jnp.int32, value.shape, 1) % width
    edge = width - 1 if offset == 1 else 0
    near = pltpu.roll(value, -offset % plane, 1)
    far = pltpu.roll(value, offset * (width - 1) % plane, 1)
    return jnp.where(lane == edge, far, near)


def part(real_imag, s, c):
    return (real_imag * 4 + s) * 3 + c


def half_part(real_imag, s, c):
    return (real_imag * 2 + s) * 3 + c


def link_reader(links_ref, direction):
    def link(row, column):
        pair = links_ref[(direction * 3 + row) * 3 + column].astype(F32)
        return (pair[0:1], pair[1:2])

    return link


def spinor_reader(ref, rows):
    def spinor(s, c):
        return (ref[part(0, s, c), rows].astype(F32), ref[part(1, s, c), rows].astype(F32))

    return spinor


def over_rows(count, step, body):
    def stage(number, carry):
        body(pl.ds(pl.multiple_of(number * step, step), step))
        return carry

    lax.fori_loop(0, count // step, stage, 0)


def copy_all(pairs, sems):
    copies = [pltpu.make_async_copy(*pair, sems.at[i]) for i, pair in enumerate(pairs)]
    for copy in copies:
        copy.start()
    return copies


def halo_kernel(fwd_hbm, links_hbm, up_ref, down_ref, fwd_ref, links_ref, sems):
    count = fwd_ref.shape[0] // 4
    quarters = [pl.ds(i * count, count) for i in range(4)]
    pairs = [(fwd_hbm.at[quarter], fwd_ref.at[quarter]) for quarter in quarters]
    for copy in copy_all([*pairs, (links_hbm, links_ref)], sems):
        copy.wait()
    link = link_reader(links_ref, 2)

    def rows_body(rows):
        spinor = spinor_reader(fwd_ref, rows)
        ahead = half_spinor(spinor, 2, -1)
        behind = colour_product(link, half_spinor(spinor, 2, 1), True)
        for s in range(2):
            for c in range(3):
                for ri in range(2):
                    place = half_part(ri, s, c)
                    up_ref[place, rows] = ahead[s][c][ri].astype(BF16)
                    down_ref[place, rows] = behind[s][c][ri].astype(BF16)

    over_rows(fwd_ref.shape[1], 16, rows_body)


SIGNS = [[1, 1, 1, 1], [1, -1, 1, -1], [1, 1, -1, -1], [1, -1, -1, 1]]


def unit_sum(q, j):
    x, y = {0: (0, 0), 3: (1, 0), 2: (0, 1), 1: (1, 1)}[j]
    first, third = q & 1, q >> 1
    matrix = BASIS[first | (first ^ x) << 1 | third << 2 | (third ^ y) << 3]
    values = [complex(matrix[s, s ^ j]) for s in range(4)]
    return (SIGNS.index([round((v / values[0]).real) for v in values]), values[0])


def times_unit(unit, value):
    real, imag = value
    if unit == 1:
        return (real, imag)
    if unit == -1:
        return (-real, -imag)
    return (-imag, real) if unit == 1j else (imag, -real)


def ring_place(place):
    return place ^ (place >> 1)


def table_place(number):
    x = (number ^ (number >> 1)) & 1
    y = ((number >> 2) ^ (number >> 3)) & 1
    q = (number & 1) | ((number >> 2) & 1) << 1
    return 4 * q + ((3 * x) ^ (2 * y))


def local_kernel(
    momenta_hbm, own_hbm, list_hbm, fwd_ref, links_ref, other_ref,
    weave_ref, left_ref, places_ref, phase_ref, momenta_ref, own_ref, list_ref, sems,
    *, width, spaces, ordered,
):
    copies = copy_all(
        ((momenta_hbm, momenta_ref), (own_hbm, own_ref), (list_hbm, list_ref)), sems
    )
    columns, plane = fwd_ref.shape[1:]
    z_place = lax.axis_index("space")
    core = lax.axis_index("spin")

    def rows_body(rows):
        spinor = spinor_reader(fwd_ref, rows)
        total = [[(0.0, 0.0) for _ in range(3)] for _ in range(4)]
        for direction in range(2):
            link = link_reader(links_ref, direction)
            along_y = direction == 1
            half = half_spinor(spinor, direction, -1)
            half = [[tuple(shifted(v, 1, along_y, width) for v in z) for z in row] for row in half]
            add_hop(total, colour_product(link, half, False), direction, -1, 1)
            half = colour_product(link, half_spinor(spinor, direction, 1), True)
            half = [[tuple(shifted(v, -1, along_y, width) for v in z) for z in row] for row in half]
            add_hop(total, half, direction, 1, -1)
        for s in range(4):
            for c in range(3):
                for ri in range(2):
                    weave_ref[part(ri, s, c), rows] = total[s][c][ri]

    over_rows(columns, 8, rows_body)

    def whole_mod(value, modulus):
        return value - modulus * jnp.floor((value + 0.5) / modulus)

    site = lax.broadcasted_iota(jnp.int32, (1, plane), 1).astype(F32)
    row_of = jnp.floor((site + 0.5) / width)
    x_of = site - width * row_of
    height = plane // width
    for copy in copies:
        copy.wait()
    for p in range(phase_ref.shape[0]):
        mom = [momenta_ref[p, axis].astype(F32) for axis in range(3)]
        frac = whole_mod(mom[0] * x_of, width) / width + whole_mod(mom[1] * row_of, height) / height
        depth = jnp.full((1, plane), mom[2] * z_place.astype(F32), F32)
        theta = 2.0 * math.pi * (whole_mod(depth, spaces) / spaces + frac)
        phase_ref[p, 0:1] = jnp.cos(theta)
        phase_ref[p, 1:2] = jnp.sin(theta)

    for k in range(list_ref.shape[0]):
        places_ref[pl.ds(k, 1)] = jnp.full((1, places_ref.shape[1]), table_place(list_ref[k]))

    moms = phase_ref.shape[0]
    block = 2 * columns // spaces if ordered else columns

    def rotate(spinor, first, mom_step, spin_step):
        for p in range(moms):
            cosine = phase_ref[p, 0:1]
            sine = phase_ref[p, 1:2]
            for s in range(4):
                at = pl.ds(pl.multiple_of(first + p * mom_step + s * spin_step, block), block)
                for c in range(3):
                    real, imag = spinor(s, c)
                    lanes = pl.ds(c * plane, plane)
                    left_ref[at, lanes] = (cosine * real - sine * imag).astype(BF16)
                    lanes = pl.ds((3 + c) * plane, plane)
                    left_ref[at, lanes] = (sine * real + cosine * imag).astype(BF16)

    for source_ref, half in ((own_ref, core), (other_ref, 1 - core)):
        for number in range(columns // block):
            spinor = spinor_reader(source_ref, pl.ds(number * block, block))
            if ordered:
                target = half * (columns // block) + number
                k = (ring_place(target) - ring_place(z_place) + spaces) % spaces
                k = jnp.where(k > 1, spaces + 1 - k, k)
                rotate(spinor, k * moms * 4 * block, 4 * block, block)
            else:
                rotate(spinor, half * columns, 8 * columns, 2 * columns)


def multiply(left_ref, right_ref, outs, first_block, moms):
    height = outs[0].shape[0]
    wide = right_ref.shape[0]
    share = moms * height
    pairs = lax.dot_general(
        left_ref[pl.ds(first_block * share, len(outs) * share)],
        right_ref[...],
        (((1,), (1,)), ((), ())),
        preferred_element_type=F32,
    )
    for number, out_ref in enumerate(outs):
        for p in range(moms):
            first = number * share + p * height
            out_ref[:, pl.ds(p * wide, wide)] = pairs[first : first + height].astype(out_ref.dtype)


def first_pairs_kernel(
    weave_ref, ahead_ref, behind_ref, links_ref, left_ref, right_ref, out_ref, *, first_block, moms
):
    columns, plane = weave_ref.shape[1:]
    wide = 4 * columns
    gamma_columns, units = unit_rows(SINGLES[2])
    step = 16

    def one_colour(c, links, first_row):
        rows = pl.ds(first_row, step)

        def half(ref, s, d):
            return tuple(ref[half_part(ri, s, d), rows].astype(F32) for ri in range(2))

        hops = []
        for s in range(2):
            real = imag = None
            for d in range(3):
                u_real, u_imag = links[d]
                h_real, h_imag = half(ahead_ref, s, d)
                part_real = u_real * h_real - u_imag * h_imag
                part_imag = u_real * h_imag + u_imag * h_real
                real = part_real if real is None else real + part_real
                imag = part_imag if imag is None else imag + part_imag
            back = half(behind_ref, s, c)
            hops.append((plus_unit((real, imag), -1, back), plus_unit((real, imag), 1, back)))
        for s in range(4):
            total = (weave_ref[part(0, s, c), rows], weave_ref[part(1, s, c), rows])
            if s < 2:
                real, imag = plus_unit(total, 1, hops[s][0])
            else:
                real, imag = plus_unit(total, -units[s], hops[gamma_columns[s]][1])
            at_real = pl.ds(s * columns + first_row, step)
            at_imag = pl.ds(wide + s * columns + first_row, step)
            first = pl.ds(c * plane, plane)
            second = pl.ds((3 + c) * plane, plane)
            right_ref[at_real, first] = real.astype(BF16)
            right_ref[at_real, second] = imag.astype(BF16)
            right_ref[at_imag, first] = imag.astype(BF16)
            right_ref[at_imag, second] = (-real).astype(BF16)

    link = link_reader(links_ref, 2)
    for c in range(3):
        links = [link(c, d) for d in range(3)]
        for first_row in range(0, columns, step):
            one_colour(c, links, first_row)
    multiply(left_ref, right_ref, [out_ref], first_block, moms)


def other_pairs_kernel(left_ref, right_ref, *out_refs, first_block, moms):
    multiply(left_ref, right_ref, out_refs, first_block, moms)


def insertion_kernel(places_ref, *rest, scaling):
    *in_refs, out_hbm, table_ref, out_ref, sems = rest
    moms, _, count, block, columns = out_ref.shape
    wide = 4 * columns
    group = lax.broadcasted_iota(jnp.int32, (1, wide), 1) // columns

    even = group % 2 == 0

    def crossed(value, s):
        if s & 1:
            value = jnp.where(
                even, pltpu.roll(value, wide - columns, 1), pltpu.roll(value, columns, 1)
            )
        if s & 2:
            value = pltpu.roll(value, 2 * columns, 1)
        return value

    places = [places_ref[pl.ds(k, 1), pl.ds(0, 1)][0, 0] for k in range(count)]

    def one_momentum(p):
        spins = []
        for s in range(4):
            both = []
            for ri in range(2):
                lanes = pl.ds((2 * p + ri) * wide, wide)
                total = None
                for ref in in_refs:
                    for lead in range(ref.shape[0]):
                        term = ref[lead, pl.ds(s * block, block), lanes].astype(F32)
                        total = term if total is None else total + term
                both.append(crossed(total, s))
            spins.append(both)
        sums = [[], []]
        for ri in range(2):
            a, b, c, d = (spins[s][ri] * scaling for s in range(4))
            near, far = (a + b, a - b), (c + d, c - d)
            sums[ri] = [near[0] + far[0], near[1] + far[1], near[0] - far[0], near[1] - far[1]]
        for j in range(4):
            moved = [[v if j == 0 else pltpu.roll(v, wide - j * columns, 1) for v in r] for r in sums]
            for q in range(4):
                number, unit = unit_sum(q, j)
                value = times_unit(unit, (moved[0][number], moved[1][number]))
                for ri in range(2):
                    table_ref[p, 4 * q + j, ri] = value[ri][:, :columns]
        for k in range(count):
            for ri in range(2):
                out_ref[p, ri, k] = table_ref[p, places[k], ri]
        output_copy(p).start()

    def output_copy(p):
        return pltpu.make_async_copy(out_ref.at[p], out_hbm.at[:, p], sems.at[p])

    for p in range(moms):
        one_momentum(p)
    for p in range(moms):
        output_copy(p).wait()


def passed_along(value, axis, steps):
    count = lax.axis_size(axis)
    pairs = [(source, (source + steps) % count) for source in range(count)]
    return lax.ppermute(value, axis, pairs)


def passed_around(value, axis, number):
    count = lax.axis_size(axis)
    steps = 1 if number == 1 else count + 1 - number
    at = {ring_place(device): device for device in range(count)}
    pairs = [(at[place], at[(place + steps) % count]) for place in range(count)]
    return lax.ppermute(value, axis, pairs)


def call(kernel, out_shape, ins, cost, outs=VMEM, **kwargs):
    many = isinstance(out_shape, (list, tuple))
    return pl.pallas_call(
        kernel,
        out_shape=out_shape,
        in_specs=ins,
        out_specs=[outs] * len(out_shape) if many else outs,
        compiler_params=pltpu.CompilerParams(vmem_limit_bytes=16 * 2**20),
        cost_estimate=pl.CostEstimate(flops=cost, bytes_accessed=2**20, transcendentals=0),
        **kwargs,
    )


def in_hbm(value):
    return pltpu.with_memory_space_constraint(value, pltpu.HBM)


def shape(dims, dtype):
    return jax.ShapeDtypeStruct(dims, dtype)


def body(backward, forward, gauge_links, momenta, gamma_list):
    _, times, _, columns, _, layers, plane = forward.shape
    assert times == 1 and layers == 1
    spaces = lax.axis_size("space")
    moms = momenta.shape[0]
    count = gamma_list.shape[0]
    block = 2 * columns // spaces
    ordered = block % 16 == 0
    fwd = jnp.transpose(forward, (0, 1, 2, 4, 5, 3, 6)).reshape(24, columns, plane)
    own = jnp.transpose(backward, (0, 1, 2, 4, 5, 3, 6)).reshape(24, columns, plane)
    links = jnp.transpose(gauge_links, (1, 2, 3, 4, 5, 0, 6)).reshape(27, 2, plane)

    other = passed_along(own, "spin", 1)
    half = shape((12, columns, plane), BF16)
    to_up, to_down, fwd_here, links_here = call(
        halo_kernel,
        [half, half] + [shape(v.shape, v.dtype) for v in (fwd, links)],
        [HBM] * 2,
        10**7,
        scratch_shapes=[pltpu.SemaphoreType.DMA((5,))],
    )(*[in_hbm(v) for v in (fwd, links)])
    behind = passed_along(to_down, "space", 1)
    ahead = passed_along(to_up, "space", -1)
    rows = 8 * columns
    weave, left, places = call(
        functools.partial(local_kernel, width=LX, spaces=spaces, ordered=ordered),
        [
            shape((24, columns, plane), F32),
            shape((moms * rows, 6 * plane), BF16),
            shape((count, plane), jnp.int32),
        ],
        [HBM, HBM, HBM, VMEM, VMEM, VMEM],
        10**8,
        scratch_shapes=[
            pltpu.VMEM((moms, 2, plane), F32),
            pltpu.SMEM(momenta.shape, jnp.int32),
            pltpu.VMEM(own.shape, BF16),
            pltpu.SMEM(gamma_list.shape, jnp.int32),
            pltpu.SemaphoreType.DMA((3,)),
        ],
    )(in_hbm(momenta), in_hbm(own), in_hbm(gamma_list), fwd_here, links_here, other)
    wide = 8 * columns
    share = rows // spaces if ordered else rows
    pair_shape = shape((share, moms * wide), BF16)
    right, first = call(
        functools.partial(first_pairs_kernel, first_block=int(ordered), moms=moms),
        [shape((wide, 6 * plane), BF16), pair_shape],
        [VMEM] * 5,
        10**9,
    )(weave, ahead, behind, links_here, left)
    if ordered:

        def more(first_block, shapes):
            kernel = functools.partial(other_pairs_kernel, first_block=first_block, moms=moms)
            return call(kernel, shapes, [VMEM] * 2, 10**9)(left, right)

        others = []
        if spaces > 2:
            others = more(2, [pair_shape] * (spaces - 2))
        blocks = [*more(0, [shape(pair_shape.shape, F32)])]
        for k, value in enumerate([first, *others], 1):
            blocks.append(passed_around(value, "space", k))
        blocks = [b[None] for b in blocks]
    else:
        split = first.reshape(4, spaces, block, moms * wide)
        split = jnp.swapaxes(split, 0, 1).reshape(spaces, 4 * block, moms * wide)
        blocks = [lax.all_to_all(split, "space", 0, 0, tiled=True)]
    scaling = 0.5 / math.sqrt(3.0 * plane * spaces)
    result = call(
        functools.partial(insertion_kernel, scaling=scaling),
        shape((2, moms, count, block, columns), F32),
        [VMEM] + [VMEM] * len(blocks),
        10**8,
        outs=HBM,
        scratch_shapes=[
            pltpu.VMEM((moms, 16, 2, block, columns), F32),
            pltpu.VMEM((moms, 2, count, block, columns), F32),
            pltpu.SemaphoreType.DMA((moms,)),
        ],
    )(places, *blocks)
    return result.reshape(2, moms, count, 1, block, columns)


def solution(mesh):
    in_specs = (
        P("parts", "tm", None, "spin", None, "space", None),
        P("parts", "tm", None, "spin", None, "space", None),
        P("parts", None, None, None, "tm", "space", None),
        P(),
        P(),
    )
    out_specs = P("parts", None, None, "tm", "space", "spin")
    return jax.shard_map(body, mesh=mesh, in_specs=in_specs, out_specs=out_specs, check_vma=False)
```

```python
import functools
import math

import jax
import jax.numpy as jnp
import numpy as np
from jax import lax
from jax.experimental import pallas as pl
from jax.experimental.pallas import tpu as pltpu
from jax.sharding import PartitionSpec as P


LX = 32
F32 = jnp.float32
BF16 = jnp.bfloat16
VMEM = pl.BlockSpec(memory_space=pltpu.VMEM)
HBM = pl.BlockSpec(memory_space=pltpu.HBM)


def gamma_tables():
    zeros = np.zeros((4, 4))
    gx_imag = np.array([[0, 0, 0, 1], [0, 0, 1, 0], [0, -1, 0, 0], [-1, 0, 0, 0]]) * 1.0
    gy_real = np.array([[0, 0, 0, -1], [0, 0, 1, 0], [0, 1, 0, 0], [-1, 0, 0, 0]]) * 1.0
    gz_imag = np.array([[0, 0, 1, 0], [0, 0, 0, -1], [-1, 0, 0, 0], [0, 1, 0, 0]]) * 1.0
    gt_real = np.array([[0, 0, 1, 0], [0, 0, 0, 1], [1, 0, 0, 0], [0, 1, 0, 0]]) * 1.0
    singles = [zeros + 1j * gx_imag, gy_real + 0j, zeros + 1j * gz_imag, gt_real + 0j]
    basis = []
    for number in range(16):
        matrix = np.eye(4) + 0j
        for which in range(4):
            if number >> which & 1:
                matrix = matrix @ singles[which]
        basis.append(matrix)
    return (singles, basis)


SINGLES, BASIS = gamma_tables()


def unit_rows(matrix):
    columns = [int(np.flatnonzero(row)[0]) for row in matrix]
    return (columns, [complex(matrix[r, c]) for r, c in enumerate(columns)])


def plus_unit(total, unit, value):
    total_real, total_imag = total
    real, imag = value
    if unit == 1:
        return (total_real + real, total_imag + imag)
    if unit == -1:
        return (total_real - real, total_imag - imag)
    if unit == 1j:
        return (total_real - imag, total_imag + real)
    return (total_real + imag, total_imag - real)


def half_spinor(spinor, direction, sign):
    columns, units = unit_rows(SINGLES[direction])
    return [
        [plus_unit(spinor(s, c), sign * units[s], spinor(columns[s], c)) for c in range(3)]
        for s in range(2)
    ]


def colour_product(link, half, dagger):
    result = []
    for colours in half:
        row = []
        for c in range(3):
            real = imag = None
            for d in range(3):
                u_real, u_imag = link(d, c) if dagger else link(c, d)
                h_real, h_imag = colours[d]
                if dagger:
                    part_real = u_real * h_real + u_imag * h_imag
                    part_imag = u_real * h_imag - u_imag * h_real
                else:
                    part_real = u_real * h_real - u_imag * h_imag
                    part_imag = u_real * h_imag + u_imag * h_real
                real = part_real if real is None else real + part_real
                imag = part_imag if imag is None else imag + part_imag
            row.append((real, imag))
        result.append(row)
    return result


def add_hop(total, half, direction, sign, weight):
    columns, units = unit_rows(SINGLES[direction])
    for c in range(3):
        for s in range(2):
            total[s][c] = plus_unit(total[s][c], weight, half[s][c])
        for s in range(2, 4):
            total[s][c] = plus_unit(total[s][c], weight * sign * units[s], half[columns[s]][c])


def shifted(value, offset, along_y, width):
    plane = value.shape[-1]
    if along_y:
        return pltpu.roll(value, -offset * width % plane, 1)
    lane = lax.broadcasted_iota(jnp.int32, value.shape, 1) % width
    edge = width - 1 if offset == 1 else 0
    near = pltpu.roll(value, -offset % plane, 1)
    far = pltpu.roll(value, offset * (width - 1) % plane, 1)
    return jnp.where(lane == edge, far, near)


def part(real_imag, s, c):
    return (real_imag * 4 + s) * 3 + c


def half_part(real_imag, s, c):
    return (real_imag * 2 + s) * 3 + c


def link_reader(links_ref, direction):
    def link(row, column):
        pair = links_ref[(direction * 3 + row) * 3 + column].astype(F32)
        return (pair[0:1], pair[1:2])

    return link


def spinor_reader(ref, rows):
    def spinor(s, c):
        return (ref[part(0, s, c), rows].astype(F32), ref[part(1, s, c), rows].astype(F32))

    return spinor


def over_rows(count, step, body):
    def stage(number, carry):
        body(pl.ds(pl.multiple_of(number * step, step), step))
        return carry

    lax.fori_loop(0, count // step, stage, 0)


def copy_all(pairs, sems):
    copies = [pltpu.make_async_copy(*pair, sems.at[i]) for i, pair in enumerate(pairs)]
    for copy in copies:
        copy.start()
    return copies


def halo_kernel(fwd_hbm, links_hbm, up_ref, down_ref, fwd_ref, links_ref, sems):
    count = fwd_ref.shape[0] // 4
    quarters = [pl.ds(i * count, count) for i in range(4)]
    pairs = [(fwd_hbm.at[quarter], fwd_ref.at[quarter]) for quarter in quarters]
    for copy in copy_all([*pairs, (links_hbm, links_ref)], sems):
        copy.wait()
    link = link_reader(links_ref, 2)

    def rows_body(rows):
        spinor = spinor_reader(fwd_ref, rows)
        ahead = half_spinor(spinor, 2, -1)
        behind = colour_product(link, half_spinor(spinor, 2, 1), True)
        for s in range(2):
            for c in range(3):
                for ri in range(2):
                    place = half_part(ri, s, c)
                    up_ref[place, rows] = ahead[s][c][ri].astype(BF16)
                    down_ref[place, rows] = behind[s][c][ri].astype(BF16)

    over_rows(fwd_ref.shape[1], 16, rows_body)


SIGNS = [[1, 1, 1, 1], [1, -1, 1, -1], [1, 1, -1, -1], [1, -1, -1, 1]]


def unit_sum(q, j):
    x, y = {0: (0, 0), 3: (1, 0), 2: (0, 1), 1: (1, 1)}[j]
    first, third = q & 1, q >> 1
    matrix = BASIS[first | (first ^ x) << 1 | third << 2 | (third ^ y) << 3]
    values = [complex(matrix[s, s ^ j]) for s in range(4)]
    return (SIGNS.index([round((v / values[0]).real) for v in values]), values[0])


def times_unit(unit, value):
    real, imag = value
    if unit == 1:
        return (real, imag)
    if unit == -1:
        return (-real, -imag)
    return (-imag, real) if unit == 1j else (imag, -real)


def ring_place(place):
    return (place & 1) * 2 + (place >> 1)


def table_place(number):
    x = (number ^ (number >> 1)) & 1
    y = ((number >> 2) ^ (number >> 3)) & 1
    q = (number & 1) | ((number >> 2) & 1) << 1
    return 4 * q + ((3 * x) ^ (2 * y))


def local_kernel(
    momenta_hbm, own_hbm, list_hbm, fwd_ref, links_ref, other_ref,
    weave_ref, left_ref, places_ref, phase_ref, momenta_ref, own_ref, list_ref, sems,
    *, width, spaces, ordered,
):
    copies = copy_all(
        ((momenta_hbm, momenta_ref), (own_hbm, own_ref), (list_hbm, list_ref)), sems
    )
    columns, plane = fwd_ref.shape[1:]
    z_place = lax.axis_index("space")
    core = lax.axis_index("spin")

    def rows_body(rows):
        spinor = spinor_reader(fwd_ref, rows)
        total = [[(0.0, 0.0) for _ in range(3)] for _ in range(4)]
        for direction in range(2):
            link = link_reader(links_ref, direction)
            along_y = direction == 1
            half = half_spinor(spinor, direction, -1)
            half = [[tuple(shifted(v, 1, along_y, width) for v in z) for z in row] for row in half]
            add_hop(total, colour_product(link, half, False), direction, -1, 1)
            half = colour_product(link, half_spinor(spinor, direction, 1), True)
            half = [[tuple(shifted(v, -1, along_y, width) for v in z) for z in row] for row in half]
            add_hop(total, half, direction, 1, -1)
        for s in range(4):
            for c in range(3):
                for ri in range(2):
                    weave_ref[part(ri, s, c), rows] = total[s][c][ri]

    over_rows(columns, 8, rows_body)

    def whole_mod(value, modulus):
        return value - modulus * jnp.floor((value + 0.5) / modulus)

    site = lax.broadcasted_iota(jnp.int32, (1, plane), 1).astype(F32)
    row_of = jnp.floor((site + 0.5) / width)
    x_of = site - width * row_of
    height = plane // width
    for copy in copies:
        copy.wait()
    for p in range(phase_ref.shape[0]):
        mom = [momenta_ref[p, axis].astype(F32) for axis in range(3)]
        frac = whole_mod(mom[0] * x_of, width) / width + whole_mod(mom[1] * row_of, height) / height
        depth = jnp.full((1, plane), mom[2] * z_place.astype(F32), F32)
        theta = 2.0 * math.pi * (whole_mod(depth, spaces) / spaces + frac)
        phase_ref[p, 0:1] = jnp.cos(theta)
        phase_ref[p, 1:2] = jnp.sin(theta)

    for k in range(list_ref.shape[0]):
        places_ref[pl.ds(k, 1)] = jnp.full((1, places_ref.shape[1]), table_place(list_ref[k]))

    moms = phase_ref.shape[0]
    block = 2 * columns // spaces if ordered else columns

    def rotate(spinor, first, mom_step, spin_step):
        for p in range(moms):
            cosine = phase_ref[p, 0:1]
            sine = phase_ref[p, 1:2]
            for s in range(4):
                at = pl.ds(pl.multiple_of(first + p * mom_step + s * spin_step, block), block)
                for c in range(3):
                    real, imag = spinor(s, c)
                    lanes = pl.ds(c * plane, plane)
                    left_ref[at, lanes] = (cosine * real - sine * imag).astype(BF16)
                    lanes = pl.ds((3 + c) * plane, plane)
                    left_ref[at, lanes] = (sine * real + cosine * imag).astype(BF16)

    for source_ref, half in ((own_ref, core), (other_ref, 1 - core)):
        for number in range(columns // block):
            spinor = spinor_reader(source_ref, pl.ds(number * block, block))
            if ordered:
                target = half * (columns // block) + number
                k = (ring_place(target) - ring_place(z_place) + spaces) % spaces
                k = jnp.where(k > 0, spaces - k, k)
                rotate(spinor, k * moms * 4 * block, 4 * block, block)
            else:
                rotate(spinor, half * columns, 8 * columns, 2 * columns)


def multiply(left_ref, right_ref, outs, first_block, moms):
    height = outs[0].shape[0]
    wide = right_ref.shape[0]
    share = moms * height
    pairs = lax.dot_general(
        left_ref[pl.ds(first_block * share, len(outs) * share)],
        right_ref[...],
        (((1,), (1,)), ((), ())),
        preferred_element_type=F32,
    )
    for number, out_ref in enumerate(outs):
        for p in range(moms):
            first = number * share + p * height
            out_ref[:, pl.ds(p * wide, wide)] = pairs[first : first + height].astype(out_ref.dtype)


def first_pairs_kernel(
    weave_ref, ahead_ref, behind_ref, links_ref, left_ref, right_ref, out_ref, *, first_block, moms
):
    columns, plane = weave_ref.shape[1:]
    wide = 4 * columns
    gamma_columns, units = unit_rows(SINGLES[2])
    step = columns

    def one_colour(c, links, first_row):
        rows = pl.ds(first_row, step)

        def half(ref, s, d):
            return tuple(ref[half_part(ri, s, d), rows].astype(F32) for ri in range(2))

        hops = []
        for s in range(2):
            real = imag = None
            for d in range(3):
                u_real, u_imag = links[d]
                h_real, h_imag = half(ahead_ref, s, d)
                part_real = u_real * h_real - u_imag * h_imag
                part_imag = u_real * h_imag + u_imag * h_real
                real = part_real if real is None else real + part_real
                imag = part_imag if imag is None else imag + part_imag
            back = half(behind_ref, s, c)
            hops.append((plus_unit((real, imag), -1, back), plus_unit((real, imag), 1, back)))
        for s in range(4):
            total = (weave_ref[part(0, s, c), rows], weave_ref[part(1, s, c), rows])
            if s < 2:
                real, imag = plus_unit(total, 1, hops[s][0])
            else:
                real, imag = plus_unit(total, -units[s], hops[gamma_columns[s]][1])
            at_real = pl.ds(s * columns + first_row, step)
            at_imag = pl.ds(wide + s * columns + first_row, step)
            first = pl.ds(c * plane, plane)
            second = pl.ds((3 + c) * plane, plane)
            right_ref[at_real, first] = real.astype(BF16)
            right_ref[at_real, second] = imag.astype(BF16)
            right_ref[at_imag, first] = imag.astype(BF16)
            right_ref[at_imag, second] = (-real).astype(BF16)

    link = link_reader(links_ref, 2)
    for c in range(3):
        links = [link(c, d) for d in range(3)]
        for first_row in range(0, columns, step):
            one_colour(c, links, first_row)
    multiply(left_ref, right_ref, [out_ref], first_block, moms)


def other_pairs_kernel(left_ref, right_ref, *out_refs, first_block, moms):
    multiply(left_ref, right_ref, out_refs, first_block, moms)


def insertion_kernel(places_ref, *rest, scaling):
    *in_refs, out_hbm, table_ref, out_ref, sems = rest
    moms, _, count, block, columns = out_ref.shape
    wide = 4 * columns
    group = lax.broadcasted_iota(jnp.int32, (1, wide), 1) // columns

    even = group % 2 == 0

    def crossed(value, s):
        if s & 1:
            value = jnp.where(
                even, pltpu.roll(value, wide - columns, 1), pltpu.roll(value, columns, 1)
            )
        if s & 2:
            value = pltpu.roll(value, 2 * columns, 1)
        return value

    places = [places_ref[pl.ds(k, 1), pl.ds(0, 1)][0, 0] for k in range(count)]

    def one_momentum(p):
        spins = []
        for s in range(4):
            both = []
            for ri in range(2):
                lanes = pl.ds((2 * p + ri) * wide, wide)
                total = None
                for ref in in_refs:
                    for lead in range(ref.shape[0]):
                        term = ref[lead, pl.ds(s * block, block), lanes].astype(F32)
                        total = term if total is None else total + term
                both.append(crossed(total, s))
            spins.append(both)
        sums = [[], []]
        for ri in range(2):
            a, b, c, d = (spins[s][ri] * scaling for s in range(4))
            near, far = (a + b, a - b), (c + d, c - d)
            sums[ri] = [near[0] + far[0], near[1] + far[1], near[0] - far[0], near[1] - far[1]]
        for j in range(4):
            moved = [[v if j == 0 else pltpu.roll(v, wide - j * columns, 1) for v in r] for r in sums]
            for q in range(4):
                number, unit = unit_sum(q, j)
                value = times_unit(unit, (moved[0][number], moved[1][number]))
                for ri in range(2):
                    table_ref[p, 4 * q + j, ri] = value[ri][:, :columns]
        for k in range(count):
            for ri in range(2):
                out_ref[p, ri, k] = table_ref[p, places[k], ri]
        output_copy(p).start()

    def output_copy(p):
        return pltpu.make_async_copy(out_ref.at[p], out_hbm.at[:, p], sems.at[p])

    for p in range(moms):
        one_momentum(p)
    for p in range(moms):
        output_copy(p).wait()


def passed_along(value, axis, steps):
    count = lax.axis_size(axis)
    pairs = [(source, (source + steps) % count) for source in range(count)]
    return lax.ppermute(value, axis, pairs)


def passed_around(value, axis, number):
    count = lax.axis_size(axis)
    steps = count - number
    at = {ring_place(device): device for device in range(count)}
    pairs = [(at[place], at[(place + steps) % count]) for place in range(count)]
    return lax.ppermute(value, axis, pairs)


def call(kernel, out_shape, ins, cost, outs=VMEM, **kwargs):
    many = isinstance(out_shape, (list, tuple))
    return pl.pallas_call(
        kernel,
        out_shape=out_shape,
        in_specs=ins,
        out_specs=[outs] * len(out_shape) if many else outs,
        compiler_params=pltpu.CompilerParams(vmem_limit_bytes=16 * 2**20),
        cost_estimate=pl.CostEstimate(flops=cost, bytes_accessed=2**20, transcendentals=0),
        **kwargs,
    )


def in_hbm(value):
    return pltpu.with_memory_space_constraint(value, pltpu.HBM)


def shape(dims, dtype):
    return jax.ShapeDtypeStruct(dims, dtype)


def body(backward, forward, gauge_links, momenta, gamma_list):
    _, times, _, columns, _, layers, plane = forward.shape
    assert times == 1 and layers == 1
    spaces = lax.axis_size("space")
    moms = momenta.shape[0]
    count = gamma_list.shape[0]
    block = 2 * columns // spaces
    ordered = block % 16 == 0
    fwd = jnp.transpose(forward, (0, 1, 2, 4, 5, 3, 6)).reshape(24, columns, plane)
    own = jnp.transpose(backward, (0, 1, 2, 4, 5, 3, 6)).reshape(24, columns, plane)
    links = jnp.transpose(gauge_links, (1, 2, 3, 4, 5, 0, 6)).reshape(27, 2, plane)

    other = passed_along(own, "spin", 1)
    half = shape((12, columns, plane), BF16)
    to_up, to_down, fwd_here, links_here = call(
        halo_kernel,
        [half, half] + [shape(v.shape, v.dtype) for v in (fwd, links)],
        [HBM] * 2,
        10**7,
        scratch_shapes=[pltpu.SemaphoreType.DMA((5,))],
    )(*[in_hbm(v) for v in (fwd, links)])
    behind = passed_along(to_down, "space", 1)
    ahead = passed_along(to_up, "space", -1)
    rows = 8 * columns
    weave, left, places = call(
        functools.partial(local_kernel, width=LX, spaces=spaces, ordered=ordered),
        [
            shape((24, columns, plane), F32),
            shape((moms * rows, 6 * plane), BF16),
            shape((count, plane), jnp.int32),
        ],
        [HBM, HBM, HBM, VMEM, VMEM, VMEM],
        10**8,
        scratch_shapes=[
            pltpu.VMEM((moms, 2, plane), F32),
            pltpu.SMEM(momenta.shape, jnp.int32),
            pltpu.VMEM(own.shape, BF16),
            pltpu.SMEM(gamma_list.shape, jnp.int32),
            pltpu.SemaphoreType.DMA((3,)),
        ],
    )(in_hbm(momenta), in_hbm(own), in_hbm(gamma_list), fwd_here, links_here, other)
    wide = 8 * columns
    share = rows // spaces if ordered else rows
    pair_shape = shape((share, moms * wide), BF16)
    right, first = call(
        functools.partial(first_pairs_kernel, first_block=int(ordered), moms=moms),
        [shape((wide, 6 * plane), BF16), pair_shape],
        [VMEM] * 5,
        10**9,
    )(weave, ahead, behind, links_here, left)
    if ordered:

        def more(first_block, shapes):
            kernel = functools.partial(other_pairs_kernel, first_block=first_block, moms=moms)
            return call(kernel, shapes, [VMEM] * 2, 10**9)(left, right)

        others = []
        if spaces > 2:
            others = more(2, [pair_shape] * (spaces - 2))
        blocks = [*more(0, [shape(pair_shape.shape, F32)])]
        for k, value in enumerate([first, *others], 1):
            blocks.append(passed_around(value, "space", k))
        blocks = [b[None] for b in blocks]
    else:
        split = first.reshape(4, spaces, block, moms * wide)
        split = jnp.swapaxes(split, 0, 1).reshape(spaces, 4 * block, moms * wide)
        blocks = [lax.all_to_all(split, "space", 0, 0, tiled=True)]
    scaling = 0.5 / math.sqrt(3.0 * plane * spaces)
    result = call(
        functools.partial(insertion_kernel, scaling=scaling),
        shape((2, moms, count, block, columns), F32),
        [VMEM] + [VMEM] * len(blocks),
        10**8,
        outs=HBM,
        scratch_shapes=[
            pltpu.VMEM((moms, 16, 2, block, columns), F32),
            pltpu.VMEM((moms, 2, count, block, columns), F32),
            pltpu.SemaphoreType.DMA((moms,)),
        ],
    )(places, *blocks)
    return result.reshape(2, moms, count, 1, block, columns)


def solution(mesh):
    in_specs = (
        P("parts", "tm", None, "spin", None, "space", None),
        P("parts", "tm", None, "spin", None, "space", None),
        P("parts", None, None, None, "tm", "space", None),
        P(),
        P(),
    )
    out_specs = P("parts", None, None, "tm", "space", "spin")
    return jax.shard_map(body, mesh=mesh, in_specs=in_specs, out_specs=out_specs, check_vma=False)
```
